32 devices in a mesh: dp: 8 (over y, x, core), mp: 4 (over z).
Axes of the slice: x: 2, y: 2, z: 4, core: 2. Of those that a mesh axis runs over, the one named last changes fastest.
Arguments:
- layer_input: bfloat16 [32, 8192], P('dp'), may hold values from -6 to 6
- pre_act: bfloat16 [32, 8192], P('dp', 'mp'), may hold values from -8 to 8
- hidden_adjoint: bfloat16 [32, 8192], P('dp', 'mp'), may hold values from -6 to 6
- output_adjoint: bfloat16 [32, 8192], P('dp', 'mp'), may hold values from -6 to 6
Outputs:
- precond_in: float32 [8192, 8192], P('dp', 'mp')
- direction_in: float32 [8192, 8192], P('dp', 'mp')
- precond_out: float32 [8192, 8192], P('dp', 'mp')
- direction_out: float32 [8192, 8192], P('dp', 'mp')
- sq_norm: float32 [], replicated
The draws below stay inside these ranges and needn't reach their ends.
All inputs are finite; a program needn't handle non-finite values.
Results may differ from the reference program's by a relative error of at most 0.0029.
Values may be sent and summed in bfloat16 or wider, within the bound.
A program may use at most 64 MiB of HBM per device.

```python
import jax
import jax.numpy as jnp

D = 8192
H = 8192
EXAMPLES = 32


def shard_levels(stream_key, dims, cuts, low, top_value):
    loudness, own = 1.0, jax.random.fold_in(stream_key, 6)
    for dim, blocks in cuts:
        draws = jnp.exp(jax.random.uniform(jax.random.fold_in(own, dim), (blocks,), jnp.float32, low / len(cuts), top_value / len(cuts)))
        loudness = loudness * jnp.repeat(draws, dims[dim] // blocks).reshape([-1 if axis == dim else 1 for axis in range(len(dims))])
    return loudness


def scatter_about(stream_key, dims, scale, limit, cuts=(), held_as=jnp.bfloat16):
    loudness = shard_levels(stream_key, dims, cuts, -0.22, 0.18) if cuts else 1.0
    result = jax.random.normal(stream_key, dims, jnp.float32) * scale * loudness
    return jnp.minimum(jnp.maximum(result, -limit), limit).astype(held_as)


def setup_inputs(seed: int = 0) -> dict:
    arg_keys = jax.random.split(jax.random.key(seed), 5)
    return {
        "layer_input": scatter_about(arg_keys[0], (EXAMPLES, D), 1.0, 6.0, ((0, 8),)),
        "pre_act": scatter_about(arg_keys[1], (EXAMPLES, H), 1.5, 8.0, ((0, 8), (1, 4))),
        "hidden_adjoint": scatter_about(arg_keys[2], (EXAMPLES, H), 1.0, 6.0, ((0, 8), (1, 4))),
        "output_adjoint": scatter_about(arg_keys[3], (EXAMPLES, D), 1.0, 6.0, ((0, 8), (1, 4))),
    }


DAMPING = 0.1
EXPONENT = 0.75

def square_bf(values):
    wide = values.astype(jnp.float32)
    return (wide * wide).astype(jnp.bfloat16)

def layer_stats(activation, adjoint, total_rows):
    gradient = jnp.dot(activation.T, adjoint, preferred_element_type=jnp.float32) / total_rows
    squares = jnp.dot(square_bf(activation).T, square_bf(adjoint), preferred_element_type=jnp.float32) / total_rows
    precond = (squares + DAMPING) ** EXPONENT
    return (gradient, precond)

def reference(layer_input, pre_act, hidden_adjoint, output_adjoint):
    total_rows = layer_input.shape[0]
    preact = pre_act.astype(jnp.float32)
    logistic = jax.nn.sigmoid(preact)
    hidden = (preact * logistic).astype(jnp.bfloat16)
    adjoint = (hidden_adjoint.astype(jnp.float32) * logistic * (1.0 + preact * (1.0 - logistic))).astype(jnp.bfloat16)
    gradient_in, precond_in = layer_stats(layer_input, adjoint, total_rows)
    gradient_out, precond_out = layer_stats(hidden, output_adjoint, total_rows)
    sq_norm = jnp.sum(gradient_in * gradient_in / precond_in) + jnp.sum(gradient_out * gradient_out / precond_out)
    rescale = jnp.sqrt(2.0 * D * H / sq_norm)
    direction_in = gradient_in / precond_in * rescale
    direction_out = gradient_out / precond_out * rescale
    return (precond_in, direction_in, precond_out, direction_out, sq_norm)
```

```python
import functools

import jax
import jax.numpy as jnp
from jax import lax
from jax.experimental import pallas as pl
from jax.experimental.pallas import tpu as pltpu
from jax.sharding import PartitionSpec as P

MESH = pl.DeviceIdType.MESH
VMEM = pl.BlockSpec(memory_space=pltpu.VMEM)

DAMPING = 0.1
WIDTH = 256


def aligned(index, size):
    return pl.ds(pl.multiple_of(index * size, size), size)


def gather_kernel(
    n, m, x_ref, pre_ref, hadj_ref, oadj_ref, x_out, h_out, a_out, o_out,
    hid, adj, x_in, h_in, a_in, o_in, wide, x_send, h_send, a_send, o_send, x_recv, h_recv, a_recv, o_recv,
):
    my_d, my_m = lax.axis_index("dp"), lax.axis_index("mp")
    share = n // m
    rows, own = x_ref.shape[0], x_out.shape[1]
    source_m = my_d // share

    barrier = pltpu.get_barrier_semaphore()
    for step in range(1, n):
        pl.semaphore_signal(
            barrier, inc=1, device_id=(lax.rem(my_d + step, n), my_m), device_id_type=MESH
        )

    @pl.when(source_m != my_m)
    def _():
        for d in range(n):
            pl.semaphore_signal(barrier, inc=1, device_id=(d, source_m), device_id_type=MESH)

    preact = pre_ref[...].astype(jnp.float32)
    logistic = jax.nn.sigmoid(preact)
    hid[...] = (preact * logistic).astype(jnp.bfloat16)
    adj[...] = (
        hadj_ref[...].astype(jnp.float32) * logistic * (1.0 + preact * (1.0 - logistic))
    ).astype(jnp.bfloat16)

    pl.semaphore_wait(barrier, (n - 1) + share * (m - 1))

    def remote(src, dst, send, recv, d, mm):
        return pltpu.make_async_remote_copy(
            src_ref=src, dst_ref=dst.at[my_d], send_sem=send, recv_sem=recv.at[my_d],
            device_id=(d, mm), device_id_type=MESH,
        )

    copies = []
    for step in range(1, n):
        d = lax.rem(my_d + step, n)
        copies.append(remote(x_ref.at[:, aligned(d, own)], x_in, x_send.at[step], x_recv, d, my_m))
        copies.append(remote(adj, a_in, a_send.at[step], a_recv, d, my_m))
    hidden_copies = []
    for j in range(share):
        for k in range(m):
            d = my_m * share + j
            copy = remote(
                hid.at[:, pl.ds(j * own, own)], h_in, h_send.at[j * m + k], h_recv, d, lax.rem(my_m + k, m)
            )
            hidden_copies.append((copy, (d != my_d) if k == 0 else None))
    late = []
    for step in range(1, n):
        d = lax.rem(my_d + step, n)
        late.append(remote(oadj_ref, o_in, o_send.at[step], o_recv, d, my_m))

    def each_hidden(act):
        for copy, condition in hidden_copies:
            if condition is None:
                act(copy)
            else:
                pl.when(condition)(functools.partial(act, copy))

    each_hidden(lambda copy: copy.start())
    for copy in copies + late:
        copy.start()

    x_in[my_d] = x_ref[:, aligned(my_d, own)]
    a_in[my_d] = adj[...]
    o_in[my_d] = oadj_ref[...]

    @pl.when(source_m == my_m)
    def _():
        h_in[my_d] = hid[:, aligned(lax.rem(my_d, share), own)]

    def arrived(buffer, recv, d):
        pltpu.make_async_copy(buffer.at[d], buffer.at[d], recv.at[d]).wait()

    for step in range(1, n):
        d = lax.rem(my_d + step, n)
        arrived(x_in, x_recv, d)
        arrived(a_in, a_recv, d)
        arrived(o_in, o_recv, d)
        arrived(h_in, h_recv, d)

    @pl.when(source_m != my_m)
    def _():
        arrived(h_in, h_recv, my_d)

    for landed, out in ((x_in, x_out), (h_in, h_out), (a_in, a_out), (o_in, o_out)):
        columns = out.shape[1]
        for d in range(n):
            wide[pl.ds(d * rows, rows), pl.ds(0, columns)] = landed[d].astype(jnp.float32)
        out[...] = wide[:, pl.ds(0, columns)].astype(jnp.bfloat16)

    for copy in copies + late:
        copy.wait_send()
    each_hidden(lambda copy: copy.wait_send())


def gather_plain(layer_input, pre_act, hidden_adjoint, output_adjoint):
    preact = pre_act.astype(jnp.float32)
    logistic = jax.nn.sigmoid(preact)
    hidden = (preact * logistic).astype(jnp.bfloat16)
    adjoint = (
        hidden_adjoint.astype(jnp.float32) * logistic * (1.0 + preact * (1.0 - logistic))
    ).astype(jnp.bfloat16)
    wide_hidden = lax.all_gather(hidden, "mp", axis=1, tiled=True)
    return (
        lax.all_to_all(layer_input, "dp", split_axis=1, concat_axis=0, tiled=True),
        lax.all_to_all(wide_hidden, "dp", split_axis=1, concat_axis=0, tiled=True),
        lax.all_gather(adjoint, "dp", axis=0, tiled=True),
        lax.all_gather(output_adjoint, "dp", axis=0, tiled=True),
    )


def square_bf(values):
    wide = values.astype(jnp.float32)
    return (wide * wide).astype(jnp.bfloat16)


def products(left, left_sq, right, total_rows):
    gradient = jnp.dot(left, right, preferred_element_type=jnp.float32) / total_rows
    squares = jnp.dot(left_sq, square_bf(right), preferred_element_type=jnp.float32) / total_rows
    damped = squares + DAMPING
    root = lax.rsqrt(damped)
    return gradient, damped, root, root * lax.rsqrt(root)


def turn(refs, turned, squared):
    @pl.when(pl.program_id(0) == 0)
    def _():
        for layer, ref in enumerate(refs):
            value = ref[...].astype(jnp.float32).T
            turned[layer] = value.astype(jnp.bfloat16)
            squared[layer] = (value * value).astype(jnp.bfloat16)


def precond_kernel(
    chunk, x_ref, h_ref, a_ref, o_ref, p_in, p_out, norm, turned, squared
):
    turn((x_ref, h_ref), turned, squared)
    total_rows = x_ref.shape[0]

    @pl.when(pl.program_id(0) == 0)
    def _():
        norm[...] = jnp.zeros_like(norm)

    for layer, (right_ref, out) in enumerate(((a_ref, p_in), (o_ref, p_out))):
        right = right_ref[...]
        total = norm[...]
        for start in range(0, out.shape[0], chunk):
            part = pl.ds(start, chunk)
            gradient, damped, root, mixed = products(
                turned[layer, part], squared[layer, part], right, total_rows
            )
            out[part, :] = damped * mixed
            term = gradient * gradient * (root * mixed)
            total = total + jnp.sum(term.reshape(chunk // 8, 8, term.shape[1]), axis=0)
        norm[...] = total


def reduce_kernel(n, m, part_ref, total_out, mine, slots, send, recv):
    my_d, my_m = lax.axis_index("dp"), lax.axis_index("mp")
    me = my_d * m + my_m
    count = n * m

    def other(step):
        peer = lax.rem(me + step, count)
        return peer, (peer // m, lax.rem(peer, m))

    barrier = pltpu.get_barrier_semaphore()
    for step in range(1, count):
        pl.semaphore_signal(barrier, inc=1, device_id=other(step)[1], device_id_type=MESH)
    column = jnp.sum(part_ref[...], axis=0, keepdims=True)
    narrow = column[:, :128]
    for start in range(128, column.shape[1], 128):
        narrow = narrow + column[:, start : start + 128]
    mine[...] = narrow
    slots[me] = narrow
    pl.semaphore_wait(barrier, count - 1)
    copies = []
    for step in range(1, count):
        copy = pltpu.make_async_remote_copy(
            src_ref=mine, dst_ref=slots.at[me], send_sem=send.at[step], recv_sem=recv.at[me],
            device_id=other(step)[1], device_id_type=MESH,
        )
        copy.start()
        copies.append(copy)
    for step in range(1, count):
        peer = other(step)[0]
        pltpu.make_async_copy(slots.at[peer], slots.at[peer], recv.at[peer]).wait()
    total = jnp.sum(slots[...], axis=0)
    total_out[...] = jnp.broadcast_to(jnp.sum(total, axis=1, keepdims=True), total_out.shape)
    for copy in copies:
        copy.wait_send()


def direction_kernel(
    chunk, entries, x_ref, h_ref, a_ref, o_ref, total_ref, d_in, d_out, norm_out, turned, squared
):
    turn((x_ref, h_ref), turned, squared)
    total_rows = x_ref.shape[0]
    norm_out[...] = total_ref[:, 0:1]
    rescale = jnp.sqrt(2.0 * entries / total_ref[:, 0:1])
    for layer, (right_ref, out) in enumerate(((a_ref, d_in), (o_ref, d_out))):
        right = right_ref[...]
        for start in range(0, out.shape[0], chunk):
            part = pl.ds(start, chunk)
            gradient, _, root, mixed = products(
                turned[layer, part], squared[layer, part], right, total_rows
            )
            out[part, :] = gradient * (root * mixed) * rescale


def shards(n, m, layer_input, pre_act, hidden_adjoint, output_adjoint):
    rows, width = layer_input.shape
    local = pre_act.shape[1]
    own = width // n
    examples = rows * n
    chunk = min(own, 128)
    bf = lambda *shape: jax.ShapeDtypeStruct(shape, jnp.bfloat16)
    sems = pltpu.SemaphoreType.DMA

    direct = own % 128 == 0
    if direct:
        gathered = pl.pallas_call(
            functools.partial(gather_kernel, n, m),
            out_shape=(bf(examples, own), bf(examples, own), bf(examples, local), bf(examples, local)),
            in_specs=[VMEM] * 4,
            out_specs=(VMEM,) * 4,
            scratch_shapes=[
                pltpu.VMEM((rows, local), jnp.bfloat16),
                pltpu.VMEM((rows, local), jnp.bfloat16),
                pltpu.VMEM((n, rows, own), jnp.bfloat16),
                pltpu.VMEM((n, rows, own), jnp.bfloat16),
                pltpu.VMEM((n, rows, local), jnp.bfloat16),
                pltpu.VMEM((n, rows, local), jnp.bfloat16),
                pltpu.VMEM((examples, local), jnp.float32),
            ]
            + [sems((n,)), sems((n,)), sems((n,)), sems((n,))]
            + [sems((n,))] * 4,
            compiler_params=pltpu.CompilerParams(
                collective_id=0, has_side_effects=True, vmem_limit_bytes=8 << 20
            ),
        )(layer_input, pre_act, hidden_adjoint, output_adjoint)
    else:
        gathered = gather_plain(layer_input, pre_act, hidden_adjoint, output_adjoint)

    whole = pl.BlockSpec((examples, own), lambda i: (0, 0))
    piece = pl.BlockSpec((examples, WIDTH), lambda i: (0, i))
    block = pl.BlockSpec((own, WIDTH), lambda i: (0, i))
    result = jax.ShapeDtypeStruct((own, local), jnp.float32)
    turned = [pltpu.VMEM((2, own, examples), jnp.bfloat16)] * 2
    local_params = pltpu.CompilerParams(
        dimension_semantics=("arbitrary",), vmem_limit_bytes=24 << 20
    )
    precond_in, precond_out, norm = pl.pallas_call(
        functools.partial(precond_kernel, chunk),
        grid=(local // WIDTH,),
        out_shape=(result, result, jax.ShapeDtypeStruct((8, WIDTH), jnp.float32)),
        in_specs=[whole, whole, piece, piece],
        out_specs=(block, block, pl.BlockSpec((8, WIDTH), lambda i: (0, 0))),
        scratch_shapes=turned,
        compiler_params=local_params,
    )(*gathered)

    if direct:
        total = pl.pallas_call(
            functools.partial(reduce_kernel, n, m),
            out_shape=jax.ShapeDtypeStruct((1, 128), jnp.float32),
            in_specs=[VMEM],
            out_specs=VMEM,
            scratch_shapes=[
                pltpu.VMEM((1, 128), jnp.float32),
                pltpu.VMEM((n * m, 1, 128), jnp.float32),
                sems((n * m,)),
                sems((n * m,)),
            ],
            compiler_params=pltpu.CompilerParams(
                collective_id=1, has_side_effects=True, vmem_limit_bytes=4 << 20
            ),
        )(norm)
    else:
        total = jnp.broadcast_to(lax.psum(jnp.sum(norm), ("dp", "mp")), (1, 128))

    direction_in, direction_out, sq_norm = pl.pallas_call(
        functools.partial(direction_kernel, chunk, float(width) * float(local * m)),
        grid=(local // WIDTH,),
        out_shape=(result, result, jax.ShapeDtypeStruct((1, 1), jnp.float32)),
        in_specs=[whole, whole, piece, piece, pl.BlockSpec((1, 128), lambda i: (0, 0))],
        out_specs=(block, block, pl.BlockSpec((1, 1), lambda i: (0, 0))),
        scratch_shapes=turned,
        compiler_params=local_params,
    )(*gathered, total)
    return (precond_in, direction_in, precond_out, direction_out, sq_norm.reshape(()))


def solution(mesh):
    placed = (P("dp", None), P("dp", "mp"), P("dp", "mp"), P("dp", "mp"))
    return jax.shard_map(
        functools.partial(shards, mesh.shape["dp"], mesh.shape["mp"]),
        mesh=mesh,
        in_specs=placed,
        out_specs=(P("dp", "mp"), P("dp", "mp"), P("dp", "mp"), P("dp", "mp"), P()),
        check_vma=False,
    )
```

```python
import functools

import jax
import jax.numpy as jnp
from jax import lax
from jax.experimental import pallas as pl
from jax.experimental.pallas import tpu as pltpu
from jax.sharding import PartitionSpec as P

MESH = pl.DeviceIdType.MESH
VMEM = pl.BlockSpec(memory_space=pltpu.VMEM)

DAMPING = 0.1
WIDTH = 256


def aligned(index, size):
    return pl.ds(pl.multiple_of(index * size, size), size)


def square_bf(values):
    wide = values.astype(jnp.float32)
    return (wide * wide).astype(jnp.bfloat16)


def mean_operand(values, total_rows):
    if total_rows & (total_rows - 1):
        return values, 1.0 / total_rows
    return values * jnp.asarray(1.0 / total_rows, values.dtype), None


def mean_product(left, right, total_rows):
    operand, factor = mean_operand(right, total_rows)
    product = jnp.dot(left, operand, preferred_element_type=jnp.float32)
    return product if factor is None else product * factor


def block_terms(left, left_sq, right, right_sq, total_rows):
    gradient = mean_product(left, right, total_rows)
    damped = mean_product(left_sq, right_sq, total_rows) + DAMPING
    root = lax.rsqrt(damped)
    return gradient, damped, root, root * lax.rsqrt(root)


def turn(value, layer, turned, squared):
    across = value.T
    turned[layer] = across.astype(jnp.bfloat16)
    squared[layer] = (across * across).astype(jnp.bfloat16)


def norm_terms(layer, turned, squared, right_ref, chunk):
    total_rows, columns = right_ref.shape
    own = turned.shape[1]

    def step(i, total):
        right = right_ref[:, aligned(i, WIDTH)]
        right_sq = square_bf(right)
        for start in range(0, own, chunk):
            part = pl.ds(start, chunk)
            gradient, _, root, mixed = block_terms(
                turned[layer, part], squared[layer, part], right, right_sq, total_rows
            )
            term = gradient * gradient * (root * mixed)
            total = total + jnp.sum(term.reshape(chunk // 8, 8, WIDTH), axis=0)
        return total

    return lax.fori_loop(0, columns // WIDTH, step, jnp.zeros((8, WIDTH), jnp.float32))


def narrowed(total):
    column = jnp.sum(total, axis=0, keepdims=True)
    narrow = column[:, :128]
    for start in range(128, column.shape[1], 128):
        narrow = narrow + column[:, start : start + 128]
    return narrow


def gather_kernel(
    n, m, chunk, x_hbm, pre_hbm, hadj_hbm, oadj_hbm, x_out, h_out, a_out, o_out, total_out,
    x_ref, pre_ref, hadj_ref, oadj_ref, hid, adj, x_in, h_in, a_in, o_in, wide, turned, squared, mine, slots,
    loads, x_send, h_send, a_send, o_send, x_recv, h_recv, a_recv, o_recv, t_send, t_recv,
):
    my_d, my_m = lax.axis_index("dp"), lax.axis_index("mp")
    share, count = n // m, n * m
    me = my_d * m + my_m
    rows, own = x_ref.shape[0], x_out.shape[1]
    source_m = my_d // share

    local_loads = [
        pltpu.make_async_copy(source, target, loads.at[i])
        for i, (source, target) in enumerate(
            ((pre_hbm, pre_ref), (hadj_hbm, hadj_ref), (x_hbm, x_ref), (oadj_hbm, oadj_ref))
        )
    ]
    for load in local_loads:
        load.start()

    def other(step):
        peer = lax.rem(me + step, count)
        return peer, (peer // m, lax.rem(peer, m))

    barrier = pltpu.get_barrier_semaphore()
    for step in range(1, count):
        pl.semaphore_signal(barrier, inc=1, device_id=other(step)[1], device_id_type=MESH)

    for load in local_loads:
        load.wait()
    preact = pre_ref[...].astype(jnp.float32)
    logistic = jax.nn.sigmoid(preact)
    hid[...] = (preact * logistic).astype(jnp.bfloat16)
    adj[...] = (
        hadj_ref[...].astype(jnp.float32) * logistic * (1.0 + preact * (1.0 - logistic))
    ).astype(jnp.bfloat16)
    x_in[my_d] = x_ref[:, aligned(my_d, own)]
    a_in[my_d] = adj[...]
    o_in[my_d] = oadj_ref[...]

    @pl.when(source_m == my_m)
    def _():
        h_in[my_d] = hid[:, aligned(lax.rem(my_d, share), own)]

    pl.semaphore_wait(barrier, count - 1)

    def remote(src, dst, send, recv, d, mm):
        return pltpu.make_async_remote_copy(
            src_ref=src, dst_ref=dst.at[my_d], send_sem=send, recv_sem=recv.at[my_d],
            device_id=(d, mm), device_id_type=MESH,
        )

    early, late, hidden_copies = [], [], []
    for step in range(1, n):
        d = lax.rem(my_d + step, n)
        early.append(remote(x_ref.at[:, aligned(d, own)], x_in, x_send.at[step], x_recv, d, my_m))
        early.append(remote(adj, a_in, a_send.at[step], a_recv, d, my_m))
        late.append(remote(oadj_ref, o_in, o_send.at[step], o_recv, d, my_m))
    for j in range(share):
        for k in range(m):
            d = my_m * share + j
            copy = remote(
                hid.at[:, pl.ds(j * own, own)], h_in, h_send.at[j * m + k], h_recv, d, lax.rem(my_m + k, m)
            )
            hidden_copies.append((copy, (d != my_d) if k == 0 else None))

    def each_hidden(act):
        for copy, condition in hidden_copies:
            if condition is None:
                act(copy)
            else:
                pl.when(condition)(functools.partial(act, copy))

    for copy in early:
        copy.start()
    each_hidden(lambda copy: copy.start())
    for copy in late:
        copy.start()

    def arrived(buffer, recv, d):
        pltpu.make_async_copy(buffer.at[d], buffer.at[d], recv.at[d]).wait()

    def assemble(landed, out):
        columns = out.shape[1]
        for d in range(n):
            wide[pl.ds(d * rows, rows), pl.ds(0, columns)] = landed[d].astype(jnp.float32)
        value = wide[:, pl.ds(0, columns)]
        out[...] = value.astype(jnp.bfloat16)
        return value

    for step in range(1, n):
        d = lax.rem(my_d + step, n)
        arrived(x_in, x_recv, d)
        arrived(a_in, a_recv, d)
    turn(assemble(x_in, x_out), 0, turned, squared)
    assemble(a_in, a_out)
    total = norm_terms(0, turned, squared, a_out, chunk)

    for step in range(1, n):
        d = lax.rem(my_d + step, n)
        arrived(h_in, h_recv, d)
        arrived(o_in, o_recv, d)

    @pl.when(source_m != my_m)
    def _():
        arrived(h_in, h_recv, my_d)

    turn(assemble(h_in, h_out), 1, turned, squared)
    assemble(o_in, o_out)
    total = total + norm_terms(1, turned, squared, o_out, chunk)

    narrow = narrowed(total)
    mine[...] = narrow
    slots[me] = narrow
    sums = []
    for step in range(1, count):
        copy = pltpu.make_async_remote_copy(
            src_ref=mine, dst_ref=slots.at[me], send_sem=t_send.at[step], recv_sem=t_recv.at[me],
            device_id=other(step)[1], device_id_type=MESH,
        )
        copy.start()
        sums.append(copy)
    for copy in early + late:
        copy.wait_send()
    each_hidden(lambda copy: copy.wait_send())
    for step in range(1, count):
        arrived(slots, t_recv, other(step)[0])
    total = jnp.sum(slots[...], axis=0)
    total_out[...] = jnp.broadcast_to(jnp.sum(total, axis=1, keepdims=True), total_out.shape)
    for copy in sums:
        copy.wait_send()


def gather_plain(layer_input, pre_act, hidden_adjoint, output_adjoint):
    preact = pre_act.astype(jnp.float32)
    logistic = jax.nn.sigmoid(preact)
    hidden = (preact * logistic).astype(jnp.bfloat16)
    adjoint = (
        hidden_adjoint.astype(jnp.float32) * logistic * (1.0 + preact * (1.0 - logistic))
    ).astype(jnp.bfloat16)
    wide_hidden = lax.all_gather(hidden, "mp", axis=1, tiled=True)
    return (
        lax.all_to_all(layer_input, "dp", split_axis=1, concat_axis=0, tiled=True),
        lax.all_to_all(wide_hidden, "dp", split_axis=1, concat_axis=0, tiled=True),
        lax.all_gather(adjoint, "dp", axis=0, tiled=True),
        lax.all_gather(output_adjoint, "dp", axis=0, tiled=True),
    )


def norm_kernel(chunk, x_ref, h_ref, a_ref, o_ref, norm, turned, squared):
    for layer, (left_ref, right_ref) in enumerate(((x_ref, a_ref), (h_ref, o_ref))):
        turn(left_ref[...].astype(jnp.float32), layer, turned, squared)
        terms = norm_terms(layer, turned, squared, right_ref, chunk)
        norm[...] = terms if layer == 0 else norm[...] + terms


def write_kernel(
    chunk, entries, x_ref, h_ref, a_ref, o_ref, total_ref, p_in, d_in, p_out, d_out, norm_out, turned, squared
):
    column, row = pl.program_id(0), pl.program_id(1)

    @pl.when((column == 0) & (row == 0))
    def _():
        norm_out[...] = total_ref[:, 0:1]
        for layer, ref in enumerate((x_ref, h_ref)):
            turn(ref[...].astype(jnp.float32), layer, turned, squared)

    total_rows = x_ref.shape[0]
    rescale = jnp.sqrt(2.0 * entries / total_ref[:, 0:1])
    height = p_in.shape[0]
    for layer, (right_ref, precond, direction) in enumerate(((a_ref, p_in, d_in), (o_ref, p_out, d_out))):
        right = right_ref[:, aligned(column, WIDTH)]
        right_sq = square_bf(right)
        for start in range(0, height, chunk):
            part = pl.ds(start, chunk)
            source = pl.ds(pl.multiple_of(row * height + start, chunk), chunk)
            gradient, damped, root, mixed = block_terms(
                turned[layer, source], squared[layer, source], right, right_sq, total_rows
            )
            precond[part, :] = damped * mixed
            direction[part, :] = gradient * (root * mixed) * rescale


def shards(n, m, layer_input, pre_act, hidden_adjoint, output_adjoint):
    rows, width = layer_input.shape
    local = pre_act.shape[1]
    own = width // n
    examples = rows * n
    chunk = min(own, 128)
    height = min(own, 512)
    bf = lambda *shape: jax.ShapeDtypeStruct(shape, jnp.bfloat16)
    vm = lambda *shape: pltpu.VMEM(shape, jnp.bfloat16)
    sems = pltpu.SemaphoreType.DMA
    turned = [vm(2, own, examples)] * 2
    local_params = pltpu.CompilerParams(vmem_limit_bytes=24 << 20)

    if own % 128 == 0:
        *gathered, total = pl.pallas_call(
            functools.partial(gather_kernel, n, m, chunk),
            out_shape=(
                bf(examples, own), bf(examples, own), bf(examples, local), bf(examples, local),
                jax.ShapeDtypeStruct((1, 128), jnp.float32),
            ),
            in_specs=[pl.BlockSpec(memory_space=pltpu.HBM)] * 4,
            out_specs=(VMEM,) * 5,
            scratch_shapes=[
                vm(rows, width), vm(rows, local), vm(rows, local), vm(rows, local),
                vm(rows, local), vm(rows, local),
                vm(n, rows, own), vm(n, rows, own), vm(n, rows, local), vm(n, rows, local),
                pltpu.VMEM((examples, local), jnp.float32),
                *turned,
                pltpu.VMEM((1, 128), jnp.float32),
                pltpu.VMEM((n * m, 1, 128), jnp.float32),
                sems((4,)),
            ]
            + [sems((n,))] * 8
            + [sems((n * m,))] * 2,
            compiler_params=pltpu.CompilerParams(
                collective_id=0, has_side_effects=True, vmem_limit_bytes=16 << 20
            ),
        )(layer_input, pre_act, hidden_adjoint, output_adjoint)
    else:
        gathered = gather_plain(layer_input, pre_act, hidden_adjoint, output_adjoint)
        norm = pl.pallas_call(
            functools.partial(norm_kernel, chunk),
            out_shape=jax.ShapeDtypeStruct((8, WIDTH), jnp.float32),
            in_specs=[VMEM] * 4,
            out_specs=VMEM,
            scratch_shapes=turned,
            compiler_params=local_params,
        )(*gathered)
        total = jnp.broadcast_to(lax.psum(jnp.sum(norm), ("dp", "mp")), (1, 128))

    block = pl.BlockSpec((height, WIDTH), lambda i, j: (j, i))
    result = jax.ShapeDtypeStruct((own, local), jnp.float32)
    *results, sq_norm = pl.pallas_call(
        functools.partial(write_kernel, chunk, float(width) * float(local * m)),
        grid=(local // WIDTH, own // height),
        out_shape=(result,) * 4 + (jax.ShapeDtypeStruct((1, 1), jnp.float32),),
        in_specs=[VMEM] * 5,
        out_specs=(block,) * 4 + (pl.BlockSpec((1, 1), lambda i, j: (0, 0)),),
        scratch_shapes=turned,
        compiler_params=local_params,
    )(*gathered, total)
    return (*results, sq_norm.reshape(()))


def solution(mesh):
    placed = (P("dp", None), P("dp", "mp"), P("dp", "mp"), P("dp", "mp"))
    return jax.shard_map(
        functools.partial(shards, mesh.shape["dp"], mesh.shape["mp"]),
        mesh=mesh,
        in_specs=placed,
        out_specs=(P("dp", "mp"), P("dp", "mp"), P("dp", "mp"), P("dp", "mp"), P()),
        check_vma=False,
    )
```

```python
import functools

import jax
import jax.numpy as jnp
from jax import lax
from jax.experimental import pallas as pl
from jax.experimental.pallas import tpu as pltpu
from jax.sharding import PartitionSpec as P

MESH = pl.DeviceIdType.MESH
VMEM = pl.BlockSpec(memory_space=pltpu.VMEM)

DAMPING = 0.1
WIDTH = 256


def aligned(index, size):
    return pl.ds(pl.multiple_of(index * size, size), size)


def square_bf(values):
    wide = values.astype(jnp.float32)
    return (wide * wide).astype(jnp.bfloat16)


def mean_operand(values, total_rows):
    if total_rows & (total_rows - 1):
        return values, 1.0 / total_rows
    return values * jnp.asarray(1.0 / total_rows, values.dtype), None


def mean_product(left, right, total_rows):
    operand, factor = mean_operand(right, total_rows)
    product = jnp.dot(left, operand, preferred_element_type=jnp.float32)
    return product if factor is None else product * factor


def block_terms(left, left_sq, right, right_sq, total_rows):
    gradient = mean_product(left, right, total_rows)
    damped = mean_product(left_sq, right_sq, total_rows) + DAMPING
    root = lax.rsqrt(damped)
    return gradient, damped, root, root * lax.rsqrt(root)


def turn(value, layer, turned, squared):
    across = value.T
    turned[layer] = across.astype(jnp.bfloat16)
    squared[layer] = (across * across).astype(jnp.bfloat16)


def norm_terms(layer, turned, squared, right_ref, chunk):
    total_rows, columns = right_ref.shape
    own = turned.shape[1]

    def step(i, total):
        right = right_ref[:, aligned(i, WIDTH)]
        right_sq = square_bf(right)
        for start in range(0, own, chunk):
            part = pl.ds(start, chunk)
            gradient, _, root, mixed = block_terms(
                turned[layer, part], squared[layer, part], right, right_sq, total_rows
            )
            term = gradient * gradient * (root * mixed)
            total = total + jnp.sum(term.reshape(chunk // 8, 8, WIDTH), axis=0)
        return total

    return lax.fori_loop(0, columns // WIDTH, step, jnp.zeros((8, WIDTH), jnp.float32))


def narrowed(total):
    column = jnp.sum(total, axis=0, keepdims=True)
    narrow = column[:, :128]
    for start in range(128, column.shape[1], 128):
        narrow = narrow + column[:, start : start + 128]
    return narrow


def gather_kernel(
    n, m, chunk, x_hbm, pre_hbm, hadj_hbm, oadj_hbm, x_dst, h_dst, a_dst, o_dst, total_out,
    x_out, h_out, a_out, o_out, x_ref, pre_ref, hadj_ref, oadj_ref, hid, adj, x_in, h_in, a_in, o_in, wide, turned, squared, mine, slots,
    loads, stores, x_send, h_send, a_send, o_send, x_recv, h_recv, a_recv, o_recv, t_send, t_recv,
):
    my_d, my_m = lax.axis_index("dp"), lax.axis_index("mp")
    share, count = n // m, n * m
    me = my_d * m + my_m
    rows, own = x_ref.shape[0], x_out.shape[1]
    source_m = my_d // share

    local_loads = [
        pltpu.make_async_copy(source, target, loads.at[i])
        for i, (source, target) in enumerate(
            ((pre_hbm, pre_ref), (hadj_hbm, hadj_ref), (x_hbm, x_ref), (oadj_hbm, oadj_ref))
        )
    ]
    for load in local_loads:
        load.start()

    def other(step):
        peer = lax.rem(me + step, count)
        return peer, (peer // m, lax.rem(peer, m))

    barrier = pltpu.get_barrier_semaphore()
    for step in range(1, count):
        pl.semaphore_signal(barrier, inc=1, device_id=other(step)[1], device_id_type=MESH)

    for load in local_loads:
        load.wait()
    preact = pre_ref[...].astype(jnp.float32)
    logistic = jax.nn.sigmoid(preact)
    hid[...] = (preact * logistic).astype(jnp.bfloat16)
    adj[...] = (
        hadj_ref[...].astype(jnp.float32) * logistic * (1.0 + preact * (1.0 - logistic))
    ).astype(jnp.bfloat16)
    x_in[my_d] = x_ref[:, aligned(my_d, own)]
    a_in[my_d] = adj[...]
    o_in[my_d] = oadj_ref[...]

    @pl.when(source_m == my_m)
    def _():
        h_in[my_d] = hid[:, aligned(lax.rem(my_d, share), own)]

    pl.semaphore_wait(barrier, count - 1)

    def remote(src, dst, send, recv, d, mm):
        return pltpu.make_async_remote_copy(
            src_ref=src, dst_ref=dst.at[my_d], send_sem=send, recv_sem=recv.at[my_d],
            device_id=(d, mm), device_id_type=MESH,
        )

    early, late, hidden_copies = [], [], []
    for step in range(1, n):
        d = lax.rem(my_d + step, n)
        early.append(remote(x_ref.at[:, aligned(d, own)], x_in, x_send.at[step], x_recv, d, my_m))
        early.append(remote(adj, a_in, a_send.at[step], a_recv, d, my_m))
        late.append(remote(oadj_ref, o_in, o_send.at[step], o_recv, d, my_m))
    for j in range(share):
        for k in range(m):
            d = my_m * share + j
            copy = remote(
                hid.at[:, pl.ds(j * own, own)], h_in, h_send.at[j * m + k], h_recv, d, lax.rem(my_m + k, m)
            )
            hidden_copies.append((copy, (d != my_d) if k == 0 else None))

    def each_hidden(act):
        for copy, condition in hidden_copies:
            if condition is None:
                act(copy)
            else:
                pl.when(condition)(functools.partial(act, copy))

    for copy in early:
        copy.start()
    for copy in early:
        copy.wait_send()
    each_hidden(lambda copy: copy.start())
    for copy in late:
        copy.start()

    def arrived(buffer, recv, d):
        pltpu.make_async_copy(buffer.at[d], buffer.at[d], recv.at[d]).wait()

    def assemble(landed, out):
        columns = out.shape[1]
        for d in range(n):
            wide[pl.ds(d * rows, rows), pl.ds(0, columns)] = landed[d].astype(jnp.float32)
        value = wide[:, pl.ds(0, columns)]
        out[...] = value.astype(jnp.bfloat16)
        return value

    stored = [
        pltpu.make_async_copy(source, target, stores.at[i])
        for i, (source, target) in enumerate(
            ((x_out, x_dst), (a_out, a_dst), (h_out, h_dst), (o_out, o_dst))
        )
    ]
    for step in range(1, n):
        d = lax.rem(my_d + step, n)
        arrived(x_in, x_recv, d)
        arrived(a_in, a_recv, d)
    turn(assemble(x_in, x_out), 0, turned, squared)
    assemble(a_in, a_out)
    stored[0].start()
    stored[1].start()
    total = norm_terms(0, turned, squared, a_out, chunk)

    for step in range(1, n):
        d = lax.rem(my_d + step, n)
        arrived(h_in, h_recv, d)
        arrived(o_in, o_recv, d)

    @pl.when(source_m != my_m)
    def _():
        arrived(h_in, h_recv, my_d)

    turn(assemble(h_in, h_out), 1, turned, squared)
    assemble(o_in, o_out)
    stored[2].start()
    stored[3].start()
    total = total + norm_terms(1, turned, squared, o_out, chunk)

    narrow = narrowed(total)
    mine[...] = narrow
    slots[me] = narrow
    sums = []
    for step in range(1, count):
        copy = pltpu.make_async_remote_copy(
            src_ref=mine, dst_ref=slots.at[me], send_sem=t_send.at[step], recv_sem=t_recv.at[me],
            device_id=other(step)[1], device_id_type=MESH,
        )
        copy.start()
        sums.append(copy)
    for copy in late:
        copy.wait_send()
    each_hidden(lambda copy: copy.wait_send())
    for copy in stored:
        copy.wait()
    for step in range(1, count):
        arrived(slots, t_recv, other(step)[0])
    total = jnp.sum(slots[...], axis=0)
    total_out[...] = jnp.broadcast_to(jnp.sum(total, axis=1, keepdims=True), total_out.shape)
    for copy in sums:
        copy.wait_send()


def gather_plain(layer_input, pre_act, hidden_adjoint, output_adjoint):
    preact = pre_act.astype(jnp.float32)
    logistic = jax.nn.sigmoid(preact)
    hidden = (preact * logistic).astype(jnp.bfloat16)
    adjoint = (
        hidden_adjoint.astype(jnp.float32) * logistic * (1.0 + preact * (1.0 - logistic))
    ).astype(jnp.bfloat16)
    wide_hidden = lax.all_gather(hidden, "mp", axis=1, tiled=True)
    return (
        lax.all_to_all(layer_input, "dp", split_axis=1, concat_axis=0, tiled=True),
        lax.all_to_all(wide_hidden, "dp", split_axis=1, concat_axis=0, tiled=True),
        lax.all_gather(adjoint, "dp", axis=0, tiled=True),
        lax.all_gather(output_adjoint, "dp", axis=0, tiled=True),
    )


def norm_kernel(chunk, x_ref, h_ref, a_ref, o_ref, norm, turned, squared):
    for layer, (left_ref, right_ref) in enumerate(((x_ref, a_ref), (h_ref, o_ref))):
        turn(left_ref[...].astype(jnp.float32), layer, turned, squared)
        terms = norm_terms(layer, turned, squared, right_ref, chunk)
        norm[...] = terms if layer == 0 else norm[...] + terms


def write_kernel(
    chunk, entries, x_hbm, h_hbm, a_hbm, o_hbm, total_hbm, p_in, d_in, p_out, d_out, norm_out,
    x_ref, h_ref, a_ref, o_ref, total_ref, turned, squared, loads,
):
    column, row = pl.program_id(0), pl.program_id(1)

    @pl.when((column == 0) & (row == 0))
    def _():
        sources = (x_hbm, h_hbm, a_hbm, o_hbm, total_hbm)
        targets = (x_ref, h_ref, a_ref, o_ref, total_ref)
        copies = [
            pltpu.make_async_copy(source, target, loads.at[i])
            for i, (source, target) in enumerate(zip(sources, targets))
        ]
        for copy in copies:
            copy.start()
        for copy in copies:
            copy.wait()
        norm_out[...] = total_ref[:, 0:1]
        for layer, ref in enumerate((x_ref, h_ref)):
            turn(ref[...].astype(jnp.float32), layer, turned, squared)

    total_rows = x_ref.shape[0]
    rescale = jnp.sqrt(2.0 * entries / total_ref[:, 0:1])
    height = p_in.shape[0]
    for layer, (right_ref, precond, direction) in enumerate(((a_ref, p_in, d_in), (o_ref, p_out, d_out))):
        right = right_ref[:, aligned(column, WIDTH)]
        right_sq = square_bf(right)
        for start in range(0, height, chunk):
            part = pl.ds(start, chunk)
            source = pl.ds(pl.multiple_of(row * height + start, chunk), chunk)
            gradient, damped, root, mixed = block_terms(
                turned[layer, source], squared[layer, source], right, right_sq, total_rows
            )
            precond[part, :] = damped * mixed
            direction[part, :] = gradient * (root * mixed) * rescale


def shards(n, m, layer_input, pre_act, hidden_adjoint, output_adjoint):
    rows, width = layer_input.shape
    local = pre_act.shape[1]
    own = width // n
    examples = rows * n
    chunk = min(own, 128)
    height = min(own, 512)
    bf = lambda *shape: jax.ShapeDtypeStruct(shape, jnp.bfloat16)
    vm = lambda *shape: pltpu.VMEM(shape, jnp.bfloat16)
    sems = pltpu.SemaphoreType.DMA
    turned = [vm(2, own, examples)] * 2
    local_params = pltpu.CompilerParams(vmem_limit_bytes=63 << 20)

    if own % 128 == 0:
        *gathered, total = pl.pallas_call(
            functools.partial(gather_kernel, n, m, chunk),
            out_shape=(
                bf(examples, own), bf(examples, own), bf(examples, local), bf(examples, local),
                jax.ShapeDtypeStruct((1, 128), jnp.float32),
            ),
            in_specs=[pl.BlockSpec(memory_space=pltpu.HBM)] * 4,
            out_specs=(pl.BlockSpec(memory_space=pltpu.HBM),) * 4 + (VMEM,),
            scratch_shapes=[
                vm(examples, own), vm(examples, own), vm(examples, local), vm(examples, local),
                vm(rows, width), vm(rows, local), vm(rows, local), vm(rows, local),
                vm(rows, local), vm(rows, local),
                vm(n, rows, own), vm(n, rows, own), vm(n, rows, local), vm(n, rows, local),
                pltpu.VMEM((examples, local), jnp.float32),
                *turned,
                pltpu.VMEM((1, 128), jnp.float32),
                pltpu.VMEM((n * m, 1, 128), jnp.float32),
                sems((4,)),
                sems((4,)),
            ]
            + [sems((n,))] * 8
            + [sems((n * m,))] * 2,
            compiler_params=pltpu.CompilerParams(
                collective_id=0, has_side_effects=True, vmem_limit_bytes=63 << 20
            ),
        )(layer_input, pre_act, hidden_adjoint, output_adjoint)
    else:
        gathered = gather_plain(layer_input, pre_act, hidden_adjoint, output_adjoint)
        norm = pl.pallas_call(
            functools.partial(norm_kernel, chunk),
            out_shape=jax.ShapeDtypeStruct((8, WIDTH), jnp.float32),
            in_specs=[VMEM] * 4,
            out_specs=VMEM,
            scratch_shapes=turned,
            compiler_params=local_params,
        )(*gathered)
        total = jnp.broadcast_to(lax.psum(jnp.sum(norm), ("dp", "mp")), (1, 128))

    block = pl.BlockSpec((height, WIDTH), lambda i, j: (j, i))
    result = jax.ShapeDtypeStruct((own, local), jnp.float32)
    *results, sq_norm = pl.pallas_call(
        functools.partial(write_kernel, chunk, float(width) * float(local * m)),
        grid=(local // WIDTH, own // height),
        out_shape=(result,) * 4 + (jax.ShapeDtypeStruct((1, 1), jnp.float32),),
        in_specs=[pl.BlockSpec(memory_space=pltpu.HBM)] * 5,
        out_specs=(block,) * 4 + (pl.BlockSpec((1, 1), lambda i, j: (0, 0)),),
        scratch_shapes=[
            vm(examples, own), vm(examples, own), vm(examples, local), vm(examples, local),
            pltpu.VMEM((1, 128), jnp.float32),
            *turned,
            sems((5,)),
        ],
        compiler_params=local_params,
    )(*gathered, total)
    return (*results, sq_norm.reshape(()))


def solution(mesh):
    placed = (P("dp", None), P("dp", "mp"), P("dp", "mp"), P("dp", "mp"))
    return jax.shard_map(
        functools.partial(shards, mesh.shape["dp"], mesh.shape["mp"]),
        mesh=mesh,
        in_specs=placed,
        out_specs=(P("dp", "mp"), P("dp", "mp"), P("dp", "mp"), P("dp", "mp"), P()),
        check_vma=False,
    )
```
